32 devices in a mesh: section: 4 (over y, x), expert: 8 (over z, core).
Axes of the slice: x: 2, y: 2, z: 4, core: 2. Of those that a mesh axis runs over, the one named last changes fastest.
Arguments:
- tokens: bfloat16 [8, 64, 2048], P(None, 'expert'), may hold values from -6 to 6
- norm_gain: float32 [2, 2048], replicated, may hold values from 0.1 to 1.9
- w_gate: bfloat16 [4, 2048, 14336], P('section', None, 'expert'), may hold values from -0.125 to 0.125
- w_up: bfloat16 [4, 2048, 14336], P('section', None, 'expert'), may hold values from -0.125 to 0.125
- w_down: bfloat16 [4, 14336, 2048], P('section', 'expert'), may hold values from -0.0625 to 0.0625
- expert_ids: int32 [2, 8, 64, 2], P(None, None, 'expert'), may hold values from 0 to 3, as said below
- slot_ids: int32 [2, 8, 64, 2], P(None, None, 'expert'), may hold values from 0 to 4, as said below
- dropped: int32 [2, 8, 64, 2], P(None, None, 'expert'), may hold values from 0 to 1, as said below
- gate_weights: float32 [2, 8, 64, 2], P(None, None, 'expert'), may hold values from 0.1 to 1
Outputs:
- states: bfloat16 [4, 8, 64, 2048], P('section', None, 'expert')
The draws below stay inside these ranges and needn't reach their ends.
Inputs may be any that keep to these rules, and one draw needn't show every extreme that they name: `expert_ids`: the two experts of a token differ. `slot_ids`: among the kept choices of the tokens of one index of expert that name one expert, the slots are 0, 1, ... up to their count less one, each once. At most 5 kept choices of the tokens of one index of expert name one expert, and a choice is dropped only where 5 kept choices of its index of expert name its expert; in each layer and micro-batch some expert receives exactly 5 kept choices from every index of expert.
All inputs are finite; a program needn't handle non-finite values.
Results may differ from the reference program's by a relative error of at most 0.025.
Values may be sent and summed in bfloat16 or wider, within the bound.
No kernel may reach another device: no remote copies, remote signals or barrier semaphores. Data moves between devices by JAX's collectives and lax.ppermute only.
A program may use at most 64 MiB of HBM per device.

```python
import jax
import jax.numpy as jnp
from jax import lax

D = 2048
FF = 7168
EXPERTS = 4
TOK_DEV = 8
MICRO = 8
LOCAL = 2
SHARDS = 4
LAYERS = 2
TOKENS = 64
CAP = 5
N_EXPERT = 8


def routing_draw(key):
    folded = jax.random.fold_in(key, 7)
    subkeys = jax.random.split(folded, 5)
    blocks = LAYERS * MICRO * N_EXPERT
    hot_expert = jax.random.randint(subkeys[4], (LAYERS * MICRO,), 0, EXPERTS)
    hot_expert = jnp.repeat(hot_expert, N_EXPERT)[:, None]
    priority = jax.vmap(lambda subkey: jax.random.permutation(subkey, TOK_DEV))(jax.random.split(subkeys[2], blocks))
    random_pick = jax.random.randint(subkeys[0], (blocks, TOK_DEV), 0, EXPERTS)
    first_pick = jnp.where(priority < CAP, hot_expert, random_pick)
    offset = jax.random.randint(subkeys[1], (blocks, TOK_DEV), 1, EXPERTS)
    second = (first_pick + offset) % EXPERTS
    chosen = jnp.stack([first_pick, second], axis=-1).astype(jnp.int32)
    prio_pair = jnp.stack([priority * 2, priority * 2 + 1], axis=-1).reshape(blocks, 2 * TOK_DEV)
    flat_ids = chosen.reshape(blocks, 2 * TOK_DEV)
    same_expert = flat_ids[:, :, None] == flat_ids[:, None, :]
    earlier = prio_pair[:, None, :] < prio_pair[:, :, None]
    rank_vals = jnp.sum((same_expert & earlier).astype(jnp.int32), axis=-1)
    drop_flag = (rank_vals >= CAP).astype(jnp.int32)
    spare_slot = jax.random.randint(subkeys[3], (blocks, 2 * TOK_DEV), 0, CAP)
    slot_vals = jnp.where(drop_flag == 1, spare_slot, rank_vals).astype(jnp.int32)
    out_shape = (LAYERS, MICRO, TOKENS, 2)
    return (chosen.reshape(out_shape), slot_vals.reshape(out_shape), drop_flag.reshape(out_shape))


def draw_expert_ids(key, part):
    return routing_draw(key)[0]


def draw_slot_ids(key, part):
    return routing_draw(key)[1]


def draw_dropped(key, part):
    return routing_draw(key)[2]


def shard_levels(stream_key, extent, shards, least, high):
    def one(axis_at, shards_of):
        steps = jax.random.uniform(jax.random.fold_in(jax.random.fold_in(stream_key, 6), axis_at), (shards_of,), jnp.float32, least / len(shards), high / len(shards))
        return jnp.repeat(jnp.exp(steps), extent[axis_at] // shards_of).reshape((-1,) + (1,) * (len(extent) - axis_at - 1))

    level = one(*shards[0])
    for cut in shards[1:]:
        level = level * one(*cut)
    return level


def gaussian(rng, dims, deviation, reach, shards=(), held_as=jnp.bfloat16):
    result = deviation * jax.random.normal(rng, dims, jnp.float32)
    if shards:
        result = result * shard_levels(rng, dims, shards, -0.22, 0.18)
    return jnp.clip(result, -reach, reach).astype(held_as)


def setup_inputs(seed: int = 0) -> dict:
    keys = jax.random.split(jax.random.key(seed), 10)
    tokens = gaussian(keys[0], (MICRO, TOKENS, D), 1.0, 6.0, ((1, 8),))
    norm_gain = jnp.clip(1.0 + 0.18 * jax.random.normal(keys[1], (LAYERS, D), jnp.float32), 0.1, 1.9)
    w_gate = gaussian(keys[2], (2 * LAYERS, D, LOCAL * FF), D ** -0.5, 0.125, ((0, 4), (2, 8)))
    w_up = gaussian(keys[3], (2 * LAYERS, D, LOCAL * FF), D ** -0.5, 0.125, ((0, 4), (2, 8)))
    w_down = gaussian(keys[4], (2 * LAYERS, LOCAL * FF, D), FF ** -0.5, 0.0625, ((0, 4), (1, 8)))
    expert_ids = draw_expert_ids(jax.random.fold_in(keys[9], 71), 0)
    slot_ids = draw_slot_ids(jax.random.fold_in(keys[9], 71), 0)
    dropped = draw_dropped(jax.random.fold_in(keys[9], 71), 0)
    gate_weights = jnp.clip(0.1 + 0.9 * jax.random.uniform(keys[8], (LAYERS, MICRO, TOKENS, 2), jnp.float32) ** shard_levels(keys[8], (LAYERS, MICRO, TOKENS, 2), ((2, 8),), -0.2, 0.2), 0.1, 1.0)
    return dict(tokens=tokens, norm_gain=norm_gain, w_gate=w_gate, w_up=w_up, w_down=w_down, expert_ids=expert_ids, slot_ids=slot_ids, dropped=dropped, gate_weights=gate_weights)


def rms_norm(values, gain_row):
    wide_vals = values.astype(jnp.float32)
    inv_scale = lax.rsqrt(lax.optimization_barrier(jnp.mean(wide_vals * wide_vals, axis=-1, keepdims=True)) + 1e-05)
    return (wide_vals * inv_scale * gain_row).astype(jnp.bfloat16)

def expert_output(rows_in, gate_cols, up_cols, down_rows):
    row_count = rows_in.shape[0]
    gate_vals = jnp.dot(rows_in, gate_cols, preferred_element_type=jnp.float32)
    up_vals = jnp.dot(rows_in, up_cols, preferred_element_type=jnp.float32)
    hidden = (jax.nn.silu(gate_vals) * up_vals).astype(jnp.bfloat16)
    pieces = hidden.reshape(row_count, SHARDS, FF // SHARDS).astype(jnp.float32)
    blocks = down_rows.reshape(SHARDS, FF // SHARDS, D).astype(jnp.float32)
    partial_value = jnp.einsum('rsf,sfd->srd', pieces, blocks).astype(jnp.bfloat16)
    partial_value = lax.optimization_barrier(partial_value)
    return lax.optimization_barrier(jnp.sum(partial_value.astype(jnp.float32), axis=0)).astype(jnp.bfloat16)

def reference(tokens, norm_gain, w_gate, w_up, w_down, expert_ids, slot_ids, dropped, gate_weights):
    slot_limit = EXPERTS * N_EXPERT * CAP
    source = (jnp.arange(TOKENS, dtype=jnp.int32) // TOK_DEV)[:, None]
    gate_all = w_gate.reshape(LAYERS, 2, D, LOCAL * FF)
    up_all = w_up.reshape(LAYERS, 2, D, LOCAL * FF)
    down_all = w_down.reshape(LAYERS, 2, LOCAL * FF, D)

    def one_layer(state, layer_args):
        gain_row, gate_pair, up_pair, down_pair, route_all, slot_all, drop_all, weigh_all = layer_args

        def one_micro(pieces):
            current, route_now, slot_now, drop_now, weigh_now = pieces
            normed = rms_norm(current, gain_row)
            target = route_now * (N_EXPERT * CAP) + source * CAP + slot_now
            target = jnp.where(drop_now == 1, slot_limit, target).astype(jnp.int32)
            buffer = jnp.zeros((slot_limit, D), jnp.bfloat16)
            buffer = buffer.at[target[:, 0]].set(normed, mode='drop')
            buffer = buffer.at[target[:, 1]].set(normed, mode='drop')
            grouped = buffer.reshape(EXPERTS, N_EXPERT * CAP, D)
            outputs = []
            for expert_at in range(EXPERTS):
                half_index = expert_at // LOCAL
                inner_index = expert_at % LOCAL
                low = inner_index * FF
                high = (inner_index + 1) * FF
                outputs.append(expert_output(grouped[expert_at], gate_pair[half_index][:, low:high], up_pair[half_index][:, low:high], down_pair[half_index][low:high]))
            produced = jnp.concatenate(outputs, axis=0)
            clipped = jnp.minimum(target, slot_limit - 1).astype(jnp.int32)
            first_half = current.astype(jnp.float32)
            full_mix = current.astype(jnp.float32)
            for member in range(2):
                picked = produced[clipped[:, member]].astype(jnp.float32)
                weighted = weigh_now[:, member:member + 1] * picked
                kept_mask = drop_now[:, member:member + 1] == 0
                first_kept = kept_mask & (route_now[:, member:member + 1] < LOCAL)
                first_half = first_half + jnp.where(first_kept, weighted, 0.0)
                full_mix = full_mix + jnp.where(kept_mask, weighted, 0.0)
            return (first_half.astype(jnp.bfloat16), full_mix.astype(jnp.bfloat16))
        half_state, new_state = lax.map(one_micro, (state, route_all, slot_all, drop_all, weigh_all))
        return (new_state, jnp.stack([half_state, new_state]))
    final_state, paired = lax.scan(one_layer, tokens, (norm_gain, gate_all, up_all, down_all, expert_ids, slot_ids, dropped, gate_weights))
    return paired.reshape(2 * LAYERS, MICRO, TOKENS, D)
```

```python
import jax
import jax.numpy as jnp
from jax import lax
from jax.experimental import pallas as pl
from jax.experimental.pallas import tpu as pltpu
from jax.sharding import PartitionSpec as P

EXPERTS = 4


def swapped(value, axis, bit):
    pairs = [(i, i ^ bit) for i in range(lax.axis_size(axis))]
    return lax.ppermute(value, axis, pairs)


def ffn_kernel(rows_ref, gate_ref, up_ref, down_ref, keep_ref, send_ref, acc_ref):
    step = pl.program_id(0)
    rows = rows_ref[...]
    gate_vals = jnp.dot(rows, gate_ref[0], preferred_element_type=jnp.float32)
    up_vals = jnp.dot(rows, up_ref[0], preferred_element_type=jnp.float32)
    hidden = (gate_vals / (1.0 + jnp.exp(-gate_vals)) * up_vals).astype(jnp.bfloat16)
    part = jnp.dot(hidden, down_ref[0], preferred_element_type=jnp.float32)

    @pl.when(step == 0)
    def _():
        acc_ref[...] = part

    @pl.when(step > 0)
    def _():
        acc_ref[...] += part

    @pl.when(step == pl.num_programs(0) - 1)
    def _():
        half = keep_ref.shape[0]
        keep_ref[...] = acc_ref[:half, :].astype(jnp.bfloat16)
        send_ref[...] = acc_ref[half:, :].astype(jnp.bfloat16)


def ffn(rows, w_gate, w_up, w_down):
    row_count, width = rows.shape
    units = w_gate.shape[2]
    block = 256
    half = jax.ShapeDtypeStruct((row_count // 2, width), jnp.bfloat16)
    half_spec = pl.BlockSpec((row_count // 2, width), lambda i: (0, 0))
    return pl.pallas_call(
        ffn_kernel,
        out_shape=(half, half),
        grid=(units // block,),
        in_specs=[
            pl.BlockSpec((row_count, width), lambda i: (0, 0)),
            pl.BlockSpec((1, width, block), lambda i: (0, 0, i)),
            pl.BlockSpec((1, width, block), lambda i: (0, 0, i)),
            pl.BlockSpec((1, block, width), lambda i: (0, i, 0)),
        ],
        out_specs=(half_spec, half_spec),
        scratch_shapes=[pltpu.VMEM((row_count, width), jnp.float32)],
        compiler_params=pltpu.CompilerParams(dimension_semantics=("arbitrary",)),
    )(rows, w_gate, w_up, w_down)


def on_device(tokens, norm_gain, w_gate, w_up, w_down, expert_ids, slot_ids, dropped, gate_weights):
    groups = lax.axis_size("expert")
    sections = lax.axis_size("section")
    section_at = lax.axis_index("section")
    expert_at = lax.axis_index("expert")
    local_count = EXPERTS // 2
    shards = groups // local_count
    micro_count, tok_rows, width = tokens.shape
    capacity = 5 * tok_rows // (2 * EXPERTS)
    layers = sections // 2
    layer_at = section_at // 2
    half_at = section_at % 2
    group_at = expert_at // shards
    gain_row = lax.dynamic_index_in_dim(norm_gain, layer_at, 0, keepdims=False)
    route = lax.dynamic_index_in_dim(expert_ids, layer_at, 0, keepdims=False)
    slot = lax.dynamic_index_in_dim(slot_ids, layer_at, 0, keepdims=False)
    drop = lax.dynamic_index_in_dim(dropped, layer_at, 0, keepdims=False)
    weigh = lax.dynamic_index_in_dim(gate_weights, layer_at, 0, keepdims=False)

    tok_total = micro_count * tok_rows
    slot_total = micro_count * capacity
    local_id = route - half_at * local_count
    owned = (drop == 0) & (local_id >= 0) & (local_id < local_count)
    relative = local_id ^ group_at
    micro_of = jnp.arange(micro_count, dtype=jnp.int32)[:, None, None]
    place = relative * slot_total + micro_of * capacity + slot
    place = jnp.where(owned, place, -1).reshape(tok_total, 2)
    columns = jnp.arange(local_count * slot_total, dtype=jnp.int32)[None, :]
    weights = weigh.reshape(tok_total, 2)
    hit_first = place[:, 0:1] == columns
    hit_second = place[:, 1:2] == columns
    mix = jnp.where(hit_first, weights[:, 0:1], 0.0) + jnp.where(hit_second, weights[:, 1:2], 0.0)
    mix_high = mix.astype(jnp.bfloat16)
    mix_low = (mix - mix_high.astype(jnp.float32)).astype(jnp.bfloat16)
    pick = (hit_first | hit_second).astype(jnp.bfloat16).T

    bits = []
    bit = shards // 2
    while bit:
        bits.append(bit)
        bit //= 2

    state = tokens.reshape(tok_total, width)
    result = jnp.zeros((tok_total, width), jnp.bfloat16)
    for layer in range(layers):
        wide = state.astype(jnp.float32)
        inv_scale = lax.rsqrt(jnp.mean(wide * wide, axis=-1, keepdims=True) + 1e-05)
        normed = (wide * inv_scale * gain_row).astype(jnp.bfloat16)
        own = jnp.dot(pick[:slot_total], normed, preferred_element_type=jnp.float32)
        away = jnp.dot(pick[slot_total:], normed, preferred_element_type=jnp.float32)
        come = swapped(away.astype(jnp.bfloat16), "expert", shards)
        rows = jnp.concatenate([own.astype(jnp.bfloat16), come])
        for bit in bits:
            rows = jnp.concatenate([rows, swapped(rows, "expert", bit)])
        keep, send = ffn(rows, w_gate, w_up, w_down)
        for bit in bits[::-1]:
            back = swapped(send, "expert", bit)
            total = (keep.astype(jnp.float32) + back.astype(jnp.float32)).astype(jnp.bfloat16)
            keep, send = total[: total.shape[0] // 2], total[total.shape[0] // 2 :]
        back = swapped(send, "expert", shards)
        produced = jnp.concatenate([keep, back])
        part = jnp.dot(mix_high, produced, preferred_element_type=jnp.float32) + jnp.dot(
            mix_low, produced, preferred_element_type=jnp.float32
        )
        other = swapped(part.astype(jnp.bfloat16), "section", 1).astype(jnp.float32)
        both = (wide + part + other).astype(jnp.bfloat16)
        shown = jnp.where(half_at == 0, (wide + part).astype(jnp.bfloat16), both)
        result = jnp.where(layer_at == layer, shown, result)
        if layer + 1 < layers:
            state = lax.ppermute(both, "section", [(i, i + 2) for i in range(sections - 2)])
    return result.reshape(1, micro_count, tok_rows, width)


def solution(mesh):
    return jax.shard_map(
        on_device,
        mesh=mesh,
        in_specs=(
            P(None, "expert", None),
            P(),
            P("section", None, "expert"),
            P("section", None, "expert"),
            P("section", "expert", None),
            P(None, None, "expert", None),
            P(None, None, "expert", None),
            P(None, None, "expert", None),
            P(None, None, "expert", None),
        ),
        out_specs=P("section", None, "expert", None),
        check_vma=False,
    )
```

```python
import jax
import jax.numpy as jnp
from jax import lax
from jax.experimental import pallas as pl
from jax.experimental.pallas import tpu as pltpu
from jax.sharding import PartitionSpec as P

EXPERTS = 4
HIDDEN_BLOCK = 256
OUT_BLOCK = 512
CHUNKS = 1
LOAD_FLOPS = 256
VMEM_LIMIT = 16 * 2**20
HOP_PIECES = 2


def swapped(value, axis, bit):
    pairs = [(i, i ^ bit) for i in range(lax.axis_size(axis))]
    return lax.ppermute(value, axis, pairs)


def added(left, right):
    return (left.astype(jnp.float32) + right.astype(jnp.float32)).astype(jnp.bfloat16)


def ffn_kernel(rows_ref, gate_ref, up_ref, down_ref, keep_ref, send_ref, hidden_ref):
    units = hidden_ref.shape[1]
    half, width = keep_ref.shape
    rows = rows_ref[...]
    block = HIDDEN_BLOCK if units % HIDDEN_BLOCK == 0 else units
    for start in range(0, units, block):
        span = slice(start, start + block)
        gate_vals = jnp.dot(rows, gate_ref[0, :, span], preferred_element_type=jnp.float32)
        up_vals = jnp.dot(rows, up_ref[0, :, span], preferred_element_type=jnp.float32)
        hidden = gate_vals / (1.0 + jnp.exp(-gate_vals)) * up_vals
        hidden_ref[:, span] = hidden.astype(jnp.bfloat16)
    hidden = hidden_ref[...]
    block = OUT_BLOCK if width % OUT_BLOCK == 0 else width
    for start in range(0, width, block):
        span = slice(start, start + block)
        part = jnp.dot(hidden, down_ref[0, :, span], preferred_element_type=jnp.float32)
        keep_ref[:, span] = part[:half].astype(jnp.bfloat16)
        send_ref[:, span] = part[half:].astype(jnp.bfloat16)


def load_kernel(source_ref, target_ref, sems):
    parts = sems.shape[0]
    size = source_ref.shape[1] // parts
    copies = [
        pltpu.make_async_copy(
            source_ref.at[:, pl.ds(i * size, size)], target_ref.at[:, pl.ds(i * size, size)], sems.at[i]
        )
        for i in range(parts)
    ]
    for copy in copies:
        copy.start()
    for copy in copies:
        copy.wait()


def loaded(weight):
    return pl.pallas_call(
        load_kernel,
        out_shape=jax.ShapeDtypeStruct(weight.shape, weight.dtype),
        in_specs=[pl.BlockSpec(memory_space=pltpu.HBM)],
        out_specs=pl.BlockSpec(memory_space=pltpu.VMEM),
        scratch_shapes=[pltpu.SemaphoreType.DMA((4,))],
        compiler_params=pltpu.CompilerParams(vmem_limit_bytes=VMEM_LIMIT),
        cost_estimate=pl.CostEstimate(
            flops=LOAD_FLOPS * weight.size, bytes_accessed=4 * weight.size, transcendentals=0
        ),
    )(weight)


def ffn(rows, w_gate, w_up, w_down):
    row_count, width = rows.shape
    units = w_gate.shape[2]
    half = jax.ShapeDtypeStruct((row_count // 2, width), jnp.bfloat16)
    near = pl.BlockSpec(memory_space=pltpu.VMEM)
    return pl.pallas_call(
        ffn_kernel,
        out_shape=(half, half),
        in_specs=[near, near, near, near],
        out_specs=(near, near),
        scratch_shapes=[pltpu.VMEM((row_count, units), jnp.bfloat16)],
        compiler_params=pltpu.CompilerParams(vmem_limit_bytes=VMEM_LIMIT),
        cost_estimate=pl.CostEstimate(
            flops=6 * row_count * width * units,
            bytes_accessed=6 * width * units,
            transcendentals=row_count * units,
        ),
    )(rows, w_gate, w_up, w_down)


def on_device(tokens, norm_gain, w_gate, w_up, w_down, expert_ids, slot_ids, dropped, gate_weights):
    groups = lax.axis_size("expert")
    sections = lax.axis_size("section")
    section_at = lax.axis_index("section")
    expert_at = lax.axis_index("expert")
    local_count = EXPERTS // 2
    shards = groups // local_count
    micro_count, tok_rows, width = tokens.shape
    capacity = 5 * tok_rows // (2 * EXPERTS)
    layers = sections // 2
    layer_at = section_at // 2
    half_at = section_at % 2
    group_at = expert_at // shards
    gain_row = lax.dynamic_index_in_dim(norm_gain, layer_at, 0, keepdims=False)
    route = lax.dynamic_index_in_dim(expert_ids, layer_at, 0, keepdims=False)
    slot = lax.dynamic_index_in_dim(slot_ids, layer_at, 0, keepdims=False)
    drop = lax.dynamic_index_in_dim(dropped, layer_at, 0, keepdims=False)
    weigh = lax.dynamic_index_in_dim(gate_weights, layer_at, 0, keepdims=False)

    chunks = CHUNKS if micro_count % CHUNKS == 0 else 1
    micros = micro_count // chunks
    tok_total = micros * tok_rows
    slot_total = -(-micros * capacity // 8) * 8
    local_id = route - half_at * local_count
    owned = (drop == 0) & (local_id >= 0) & (local_id < local_count)
    relative = local_id ^ group_at
    micro_of = (jnp.arange(micro_count, dtype=jnp.int32) % micros)[:, None, None]
    place = relative * slot_total + micro_of * capacity + slot
    place = jnp.where(owned, place, -1).reshape(micro_count * tok_rows, 2)
    columns = jnp.arange(local_count * slot_total, dtype=jnp.int32)[None, :]
    weights = weigh.reshape(micro_count * tok_rows, 2)
    hit_first = place[:, 0:1] == columns
    hit_second = place[:, 1:2] == columns
    mix_all = jnp.where(hit_first, weights[:, 0:1], 0.0) + jnp.where(hit_second, weights[:, 1:2], 0.0)
    high_all = mix_all.astype(jnp.bfloat16)
    low_all = (mix_all - high_all.astype(jnp.float32)).astype(jnp.bfloat16)
    pick_all = (hit_first | hit_second).astype(jnp.bfloat16)

    bits = []
    bit = shards // 2
    while bit:
        bits.append(bit)
        bit //= 2

    def dispatch(state, part_at):
        wide = state.astype(jnp.float32)
        inv_scale = lax.rsqrt(jnp.mean(wide * wide, axis=-1, keepdims=True) + 1e-05)
        normed = (wide * inv_scale * gain_row).astype(jnp.bfloat16)
        pick = pick_all[part_at * tok_total : (part_at + 1) * tok_total].T
        own = jnp.dot(pick[:slot_total], normed, preferred_element_type=jnp.float32)
        away = jnp.dot(pick[slot_total:], normed, preferred_element_type=jnp.float32)
        come = swapped(away.astype(jnp.bfloat16), "expert", shards)
        own = own.astype(jnp.bfloat16)
        if not bits:
            return jnp.concatenate([own, come])
        near = swapped(own, "expert", bits[0])
        far = swapped(come, "expert", bits[0])
        rows = jnp.concatenate([own, come, near, far])
        for bit in bits[1:]:
            rows = jnp.concatenate([rows, swapped(rows, "expert", bit)])
        return rows

    def give_back(keep, send, part_at):
        for at, bit in enumerate(bits[::-1]):
            if at + 1 < len(bits):
                total = added(keep, swapped(send, "expert", bit))
                keep, send = jnp.split(total, 2)
            else:
                keep_own, keep_away = jnp.split(keep, 2)
                send_own, send_away = jnp.split(send, 2)
                send = added(keep_away, swapped(send_away, "expert", bit))
                keep = added(keep_own, swapped(send_own, "expert", bit))
        back = swapped(send, "expert", shards)
        produced = jnp.concatenate([keep, back])
        span = slice(part_at * tok_total, (part_at + 1) * tok_total)
        return jnp.dot(high_all[span], produced, preferred_element_type=jnp.float32) + jnp.dot(
            low_all[span], produced, preferred_element_type=jnp.float32
        )

    states = [tokens[c * micros : (c + 1) * micros].reshape(tok_total, width) for c in range(chunks)]
    results = [jnp.zeros((tok_total, width), jnp.bfloat16)] * chunks
    part = None
    for layer in range(layers):
        stored = (w_gate, w_up, w_down)
        if part is not None:
            stored, part = lax.optimization_barrier((stored, part))
        gate_near, up_near, down_near = [loaded(weight) for weight in stored]
        for c in range(chunks):
            rows = dispatch(states[c], c)
            keep, send = ffn(rows, gate_near, up_near, down_near)
            part = give_back(keep, send, c)
            wide = states[c].astype(jnp.float32)
            sums = []
            passed = []
            pieces = HOP_PIECES if tok_total % (8 * HOP_PIECES) == 0 else 1
            for mine, base in zip(jnp.split(part, pieces), jnp.split(wide, pieces)):
                other = swapped(mine.astype(jnp.bfloat16), "section", 1).astype(jnp.float32)
                both = (base + mine + other).astype(jnp.bfloat16)
                sums.append(both)
                if layer + 1 < layers:
                    passed.append(lax.ppermute(both, "section", [(i, i + 2) for i in range(sections - 2)]))
            both = jnp.concatenate(sums)
            shown = jnp.where(half_at == 0, (wide + part).astype(jnp.bfloat16), both)
            results[c] = jnp.where(layer_at == layer, shown, results[c])
            if layer + 1 < layers:
                states[c] = jnp.concatenate(passed)
    result = jnp.concatenate(results)
    return result.reshape(1, micro_count, tok_rows, width)


def solution(mesh):
    return jax.shard_map(
        on_device,
        mesh=mesh,
        in_specs=(
            P(None, "expert", None),
            P(),
            P("section", None, "expert"),
            P("section", None, "expert"),
            P("section", "expert", None),
            P(None, None, "expert", None),
            P(None, None, "expert", None),
            P(None, None, "expert", None),
            P(None, None, "expert", None),
        ),
        out_specs=P("section", None, "expert", None),
        check_vma=False,
    )
```
